32 devices in a mesh: island: 4 (over z), fsdp: 8 (over y, x, core).
Axes of the slice: x: 2, y: 2, z: 4, core: 2. Of those that a mesh axis runs over, the one named last changes fastest.
Arguments:
- grads: bfloat16 [4, 1, 14336, 4096], P('island', None, 'fsdp'), may hold values from -200 to 200
- buffer: bfloat16 [4, 14336, 4096], P('island', 'fsdp'), may hold values from -200 to 200
- q_old: float32 [4, 4096, 128], P('island', 'fsdp'), may hold values from -0.09375 to 0.09375
- anchor: bfloat16 [14336, 4096], P('fsdp'), may hold values from -6 to 6
- momentum: float32 [14336, 4096], P(('fsdp', 'island')), may hold values from -6 to 6
Outputs:
- anchor_new: bfloat16 [14336, 4096], P('fsdp')
- buffer_new: bfloat16 [4, 14336, 4096], P('island', 'fsdp')
- momentum_new: float32 [14336, 4096], P(('fsdp', 'island'))
The draws below stay inside these ranges and needn't reach their ends.
All inputs are finite; a program needn't handle non-finite values.
Results may differ from the reference program's by a relative error of at most 0.012.
Values may be sent and summed in bfloat16 or wider, within the bound.
No kernel may reach another device: no remote copies, remote signals or barrier semaphores. Data moves between devices by JAX's collectives and lax.ppermute only.
A program may use at most 192 MiB of HBM per device.

```python
import math
import jax
import jax.numpy as jnp
from jax import lax

ROWS = 14336
COLS = 4096
RANK = 128
STEPS = 1
ISLANDS = 4
N_ISLAND = 4


def scale_tables(key):
    base_key = jax.random.fold_in(key, 7)
    row_key, col_key = jax.random.split(base_key)
    rising_rows = 10.0 ** (jnp.arange(ROWS, dtype=jnp.float32) / ROWS)
    rising_cols = 10.0 ** (jnp.arange(COLS, dtype=jnp.float32) / COLS)
    row_scale = rising_rows * jax.random.uniform(row_key, (ROWS,), jnp.float32, 1.0, 2.0) / 5.0
    col_scale = rising_cols * jax.random.uniform(col_key, (COLS,), jnp.float32, 1.0, 2.0) / 5.0
    return (row_scale, col_scale)


def scaled_noise(key, salt, layers):
    noise_key = jax.random.fold_in(key, salt)
    row_scale, col_scale = scale_tables(key)
    shape = (ISLANDS, layers, ROWS, COLS)
    values = jnp.clip(jax.random.normal(noise_key, shape, jnp.float32), -4.0, 4.0)
    return values * row_scale[:, None] * col_scale[None, :]


def draw_grads(key, part):
    return scaled_noise(key, 21, STEPS).astype(jnp.bfloat16)


def draw_buffer(key, part):
    return scaled_noise(key, 22, 1).reshape(ISLANDS, ROWS, COLS).astype(jnp.bfloat16)


def levels(key, dims, shards, low, high):
    factor_of, own = 1.0, jax.random.fold_in(key, 6)
    for axis_at, shards_of in shards:
        draws = jnp.exp(jax.random.uniform(jax.random.fold_in(own, axis_at), (shards_of,), jnp.float32, low / len(shards), high / len(shards)))
        factor_of = factor_of * jnp.repeat(draws, dims[axis_at] // shards_of).reshape([-1 if axis == axis_at else 1 for axis in range(len(dims))])
    return factor_of


def centred(rng, extent, spread, most, cuts=(), held_as=jnp.bfloat16):
    values = spread * jax.random.normal(rng, extent, jnp.float32)
    if cuts:
        values = values * levels(rng, extent, cuts, -0.22, 0.18)
    return jnp.clip(values, -most, most).astype(held_as)


def setup_inputs(seed: int = 0) -> dict:
    keys = jax.random.split(jax.random.key(seed), 6)
    grads = draw_grads(jax.random.fold_in(keys[5], 71), 0)
    buffer = draw_buffer(jax.random.fold_in(keys[5], 71), 0)
    q_old = centred(keys[2], (ISLANDS, COLS, RANK), COLS ** -0.5, 0.09375, ((0, 4), (1, 8)), jnp.float32)
    anchor = centred(keys[3], (ROWS, COLS), 1.0, 6.0, ((0, 8),))
    momentum = centred(keys[4], (ROWS, COLS), 1.0, 6.0, ((0, 32),), jnp.float32)
    return {"grads": grads, "buffer": buffer, "q_old": q_old, "anchor": anchor, "momentum": momentum}


precise = lax.Precision.HIGHEST
error_decay = 0.95
outer_beta = 0.9
outer_rate = 0.7
epsilon = 1e-06

def product(left_side, right_side, left_dims, right_dims):
    return lax.dot_general(left_side.astype(jnp.float32), right_side.astype(jnp.float32), (((left_dims,), (right_dims,)), ((), ())), precision=precise, preferred_element_type=jnp.float32)

def inverse_upper(lower_factor):
    identity = jnp.eye(lower_factor.shape[0], dtype=lower_factor.dtype)
    return lax.linalg.triangular_solve(lower_factor, identity, left_side=True, lower=True, transpose_a=True)

def island_window(island_args):
    grad_steps, buffer_one, q_basis = island_args
    residue = buffer_one.astype(jnp.float32)
    moved_sum = jnp.zeros(residue.shape, jnp.float32)
    rate = math.sqrt(ROWS * COLS / RANK)
    for step_index in range(STEPS):
        matrix = residue + grad_steps[step_index].astype(jnp.float32)
        raw_image = product(matrix, q_basis, 1, 0)
        gram_matrix = product(raw_image, raw_image, 0, 0)
        upper_inverse = inverse_upper(jnp.linalg.cholesky(gram_matrix))
        basis_rows = product(raw_image, upper_inverse, 1, 0)
        factor = product(matrix, basis_rows, 0, 0)
        q_basis = factor / jnp.sqrt(lax.optimization_barrier(jnp.sum(factor * factor, axis=0)) + epsilon)
        residue = matrix - (1.0 - error_decay) * product(basis_rows, factor, 1, 1)
        moved_sum = moved_sum + rate * product(basis_rows, q_basis, 1, 1)
    return (moved_sum.astype(jnp.bfloat16), residue.astype(jnp.bfloat16))

def reference(grads, buffer, q_old, anchor, momentum):
    deltas, residues = lax.map(island_window, (grads, buffer, q_old))
    delta_total = lax.optimization_barrier(jnp.sum(deltas, axis=0, dtype=jnp.float32))
    delta_mean = delta_total / N_ISLAND
    momentum_new = outer_beta * momentum + delta_mean
    anchor_new = (anchor.astype(jnp.float32) - outer_rate * (delta_mean + outer_beta * momentum_new)).astype(jnp.bfloat16)
    return (anchor_new, residues, momentum_new)
```

```python
import functools
import math

import jax
import jax.numpy as jnp
from jax import lax
from jax.experimental import pallas as pl
from jax.experimental.pallas import tpu as pltpu
from jax.sharding import PartitionSpec as P


precise = lax.Precision.HIGHEST
error_decay = 0.95
outer_beta = 0.9
outer_rate = 0.7
epsilon = 1e-06
bf16 = jnp.bfloat16
f32 = jnp.float32


def params(mib):
    return pltpu.CompilerParams(
        dimension_semantics=("arbitrary",), vmem_limit_bytes=mib * 1024 * 1024
    )


def cost(flops, moved):
    return pl.CostEstimate(flops=int(flops), bytes_accessed=int(moved), transcendentals=0)


def divisor(total, most, step):
    return max(d for d in range(step, most + 1, step) if total % d == 0)


def project_kernel(slots, g_ref, b_ref, q_ref, raw_ref, proj_ref, gram_ref, q_scratch):
    blocks, width, _ = q_ref.shape

    @pl.when(pl.program_id(0) == 0)
    def _():
        proj_ref[...] = jnp.zeros_like(proj_ref)
        gram_ref[...] = jnp.zeros_like(gram_ref)
        for j in range(blocks):
            q_scratch[j * width : (j + 1) * width, :] = q_ref[slots[j]]

    matrix = g_ref[...] + b_ref[...]
    raw = jnp.dot(matrix, q_scratch[...], preferred_element_type=f32)
    raw_ref[...] = raw
    turned = raw.T
    gram_ref[...] += jnp.dot(turned, raw, precision=precise, preferred_element_type=f32)
    turned = turned.astype(bf16)
    for j in range(blocks):
        proj_ref[slots[j]] += jnp.dot(
            turned, matrix[:, j * width : (j + 1) * width], preferred_element_type=f32
        )


def project(slots, grads, buffer, q_stack):
    rows, cols = grads.shape
    blocks, width, rank = q_stack.shape
    step = divisor(rows, 256, 8)
    tile = pl.BlockSpec((step, cols), lambda i, s: (i, 0))
    whole = lambda shape: pl.BlockSpec(shape, lambda i, s: (0,) * len(shape))
    return pl.pallas_call(
        project_kernel,
        grid_spec=pltpu.PrefetchScalarGridSpec(
            num_scalar_prefetch=1,
            grid=(rows // step,),
            in_specs=[tile, tile, whole((blocks, width, rank))],
            out_specs=[
                pl.BlockSpec((step, rank), lambda i, s: (i, 0)),
                whole((blocks, rank, width)),
                whole((rank, rank)),
            ],
            scratch_shapes=[pltpu.VMEM((cols, rank), bf16)],
        ),
        out_shape=[
            jax.ShapeDtypeStruct((rows, rank), f32),
            jax.ShapeDtypeStruct((blocks, rank, width), f32),
            jax.ShapeDtypeStruct((rank, rank), f32),
        ],
        compiler_params=params(48),
        cost_estimate=cost(4 * rows * cols * rank, 4 * rows * cols),
        name="project",
    )(slots, grads, buffer, q_stack)


def residue_kernel(slots, g_ref, b_ref, p_ref, r_ref, out_ref):
    blocks, _, width = r_ref.shape
    basis = p_ref[...]
    for j in range(blocks):
        at = slice(j * width, (j + 1) * width)
        update = jnp.dot(basis, r_ref[slots[j]], preferred_element_type=f32)
        matrix = g_ref[:, at].astype(f32) + b_ref[:, at].astype(f32)
        out_ref[:, at] = (matrix - (1.0 - error_decay) * update).astype(bf16)


def residue(slots, grads, buffer, basis, stack):
    rows, cols = grads.shape
    blocks, _, width = stack.shape
    rank = basis.shape[1]
    step = divisor(rows, 256, 8)
    tile = pl.BlockSpec((step, cols), lambda i, s: (i, 0))
    return pl.pallas_call(
        residue_kernel,
        grid_spec=pltpu.PrefetchScalarGridSpec(
            num_scalar_prefetch=1,
            grid=(rows // step,),
            in_specs=[
                tile,
                tile,
                pl.BlockSpec((step, rank), lambda i, s: (i, 0)),
                pl.BlockSpec((blocks, rank, width), lambda i, s: (0, 0, 0)),
            ],
            out_specs=tile,
        ),
        out_shape=jax.ShapeDtypeStruct((rows, cols), bf16),
        compiler_params=params(48),
        cost_estimate=cost(2 * rows * cols * rank, 6 * rows * cols),
        name="residue",
    )(slots, grads, buffer, basis, stack)


def outer(momentum, anchor, mean):
    momentum_new = outer_beta * momentum + mean
    anchor_new = anchor.astype(f32) - outer_rate * (mean + outer_beta * momentum_new)
    return momentum_new, anchor_new.astype(bf16)


def scaled(rows, scale):
    return (rows.astype(f32) * scale).astype(bf16)


def change(left, low_ref, high_ref):
    depth = low_ref.shape[1]
    return jnp.dot(left[:, :depth], low_ref[0], preferred_element_type=f32) + jnp.dot(
        left[:, depth:], high_ref[0], preferred_element_type=f32
    )


def late_kernel(n, scalars, *refs):
    p_refs, (scale, low, high, m_ref, a_ref), refs = refs[:n], refs[n : n + 5], refs[n + 5 :]
    m_out, a_out, share, left = refs[-4:]
    rank = p_refs[0].shape[-1]

    @pl.when(pl.program_id(0) == 0)
    def _():
        for d in range(n):
            at = slice(d * rank, (d + 1) * rank)
            left[:, at] = scaled(p_refs[d][0, 0] if d == 0 else p_refs[d][0], scale[:, at])

    momentum_new, anchor_new = outer(m_ref[0], a_ref[0, 0], change(left, low, high))
    m_out[0] = momentum_new
    a_out[0, 0] = anchor_new
    share[...] = anchor_new


def stack_specs(stacks, start):
    blocks = stacks[0].shape[0]
    return [
        pl.BlockSpec(
            (1, *stack.shape[1:]), lambda j, s, k=k: (s[1 + k * blocks + start + j], 0, 0)
        )
        for k, stack in enumerate(stacks)
    ]


def late(scalars, own, others, scale, stacks, momentum, anchor, span, filled):
    n, parts, height, _ = anchor.shape
    width, depth, rank = stacks[0].shape[-1], scale.shape[-1], own.shape[-1]
    last, (start, stop) = parts - 1, span
    fixed = lambda *at: (lambda j, s: at)
    m_spec = pl.BlockSpec((1, height, width), lambda j, s: (last, 0, start + j))
    a_spec = pl.BlockSpec((1, 1, height, width), lambda j, s: (s[0], last, 0, start + j))
    columns = (stop - start) * width
    return pl.pallas_call(
        functools.partial(late_kernel, n),
        grid_spec=pltpu.PrefetchScalarGridSpec(
            num_scalar_prefetch=1,
            grid=(stop - start,),
            in_specs=[pl.BlockSpec((1, 1, height, rank), lambda j, s: (s[0], last, 0, 0))]
            + [pl.BlockSpec((1, height, rank), fixed(last * n, 0, 0))] * (n - 1)
            + [pl.BlockSpec((1, depth), fixed(0, 0)), *stack_specs(stacks, start), m_spec, a_spec]
            + [pl.BlockSpec(memory_space=pl.ANY)] * len(filled),
            out_specs=[m_spec, a_spec, pl.BlockSpec((height, width), lambda j, s: (0, j))],
            scratch_shapes=[pltpu.VMEM((height, depth), bf16)],
        ),
        out_shape=[
            jax.ShapeDtypeStruct(momentum.shape, f32),
            jax.ShapeDtypeStruct(anchor.shape, bf16),
            jax.ShapeDtypeStruct((height, columns), bf16),
        ],
        input_output_aliases={n + 6 + k: k for k in range(len(filled))},
        compiler_params=params(48),
        cost_estimate=cost(2 * height * columns * depth, 14 * height * columns),
        name="late",
    )(scalars, own, *others, scale, *stacks, momentum, anchor, *filled)


def early_kernel(n, counts, scalars, *refs):
    p_refs, refs = refs[:n], refs[n:]
    (scale, low, high, m_ref, a_ref), refs = refs[:5], refs[5:]
    got, refs = refs[: sum(counts)], refs[sum(counts) :]
    _, _, m_out, a_out, left, mean = refs
    rank, height = p_refs[0].shape[-1], p_refs[0].shape[-2]

    @pl.when(pl.program_id(0) == 0)
    def _():
        for d in range(n):
            at = slice(d * rank, (d + 1) * rank)
            for k in range(n):
                rows = p_refs[d][k, 0] if d == 0 else p_refs[d][k]
                left[k * height : (k + 1) * height, at] = scaled(rows, scale[:, at])

    mean[...] = change(left, low, high).reshape(mean.shape)
    for d in range(n):
        k = lax.rem(scalars[0] + d, n)
        if d == 0:
            momentum = m_ref[0]
        else:
            start = sum(counts[: d - 1])
            momentum = got[start][...].astype(f32)
            for ref in got[start + 1 : start + counts[d - 1]]:
                momentum = momentum + ref[...].astype(f32)
        momentum_new, anchor_new = outer(momentum, a_ref[k, 0], mean[k])
        if d == 0:
            m_out[0] = momentum_new
        a_out[k, 0] = anchor_new


def early(scalars, own, others, scale, stacks, momentum, anchor, got, filled):
    n, _, height, cols = anchor.shape
    blocks, _, width = stacks[0].shape
    depth, rank = scale.shape[-1], own.shape[-1]
    counts = [len(pieces) for pieces in got]
    flat = [piece for pieces in got for piece in pieces]
    fixed = lambda *at: (lambda j, s: at)
    m_spec = pl.BlockSpec((1, height, width), lambda j, s: (0, 0, j))
    a_spec = pl.BlockSpec((n, 1, height, width), lambda j, s: (0, 0, 0, j))
    first_alias = n + 6 + len(flat)
    return pl.pallas_call(
        functools.partial(early_kernel, n, counts),
        grid_spec=pltpu.PrefetchScalarGridSpec(
            num_scalar_prefetch=1,
            grid=(blocks,),
            in_specs=[pl.BlockSpec((n, 1, height, rank), fixed(0, 0, 0, 0))]
            + [pl.BlockSpec((n, height, rank), fixed(0, 0, 0))] * (n - 1)
            + [pl.BlockSpec((1, depth), fixed(0, 0)), *stack_specs(stacks, 0), m_spec, a_spec]
            + [pl.BlockSpec((height, width), lambda j, s: (0, j))] * len(flat)
            + [pl.BlockSpec(memory_space=pl.ANY)] * 2,
            out_specs=[m_spec, a_spec],
            scratch_shapes=[
                pltpu.VMEM((n * height, depth), bf16),
                pltpu.VMEM((n, height, width), f32),
            ],
        ),
        out_shape=[
            jax.ShapeDtypeStruct(momentum.shape, f32),
            jax.ShapeDtypeStruct(anchor.shape, bf16),
        ],
        input_output_aliases={first_alias: 0, first_alias + 1: 1},
        compiler_params=params(56),
        cost_estimate=cost(2 * n * height * cols * depth, 32 * height * cols),
        name="early",
    )(scalars, own, *others, scale, *stacks, momentum, anchor, *flat, *filled)


def swap(x, bit):
    size = lax.axis_size("fsdp")
    return lax.ppermute(x, "fsdp", [(i, i ^ bit) for i in range(size)])


def spread(x, bits):
    for bit in bits:
        x = jnp.concatenate([x, swap(x, bit)], axis=0)
    return x


def places(apart, bits):
    return functools.reduce(
        jnp.bitwise_or,
        [((apart >> bit.bit_length() - 1) & 1) << k for k, bit in enumerate(bits)],
        jnp.zeros_like(apart),
    )


def from_island(x, ahead):
    n = lax.axis_size("island")
    return lax.ppermute(x, "island", [(s, (s - ahead) % n) for s in range(n)])


def near(x):
    return from_island(x, 1), from_island(x, lax.axis_size("island") - 1)


def onward(above, below):
    down = lax.ppermute(above, "island", [(1, 0), (2, 1)])
    up = lax.ppermute(below, "island", [(1, 2), (2, 3)])
    return down, up


def line_step(down, up, step):
    n = lax.axis_size("island")
    down = lax.ppermute(down, "island", [(k, k - 1) for k in range(1, n - step + 1)])
    up = lax.ppermute(up, "island", [(k, k + 1) for k in range(step - 1, n - 1)])
    return down, up


def tie(*values):
    return lax.optimization_barrier(values)


def exact(a, b):
    return jnp.dot(a, b, precision=precise, preferred_element_type=f32)


def body(grads, buffer, q_old, anchor, momentum):
    n, size = lax.axis_size("island"), lax.axis_size("fsdp")
    island, place = lax.axis_index("island"), lax.axis_index("fsdp")
    grads, buffer, q_old = grads[0, 0], buffer[0], q_old[0]
    rows, cols = grads.shape
    rank = q_old.shape[1]
    rate = math.sqrt(rows * size * cols / rank)

    quarter = momentum.shape[0]
    parts = 2 if quarter % 16 == 0 else 1
    height = quarter // parts
    momentum = momentum.reshape(parts, height, cols)
    anchor = anchor.reshape(n, parts, height, cols)
    forward = n == 4
    if parts == 2:
        ahead = momentum[0].astype(bf16)
        got = near(ahead) if forward else [from_island(ahead, d) for d in range(1, n)]

    bits = [1 << k for k in range(size.bit_length() - 1)]
    split = size == 1 << len(bits) and (cols // size) % 128 == 0
    q_own = q_old.astype(bf16)
    if split:
        falling = bits[::-1]
        crossed = falling[1::-1] + falling[2:]
        q_stack = spread(q_own[None], falling)
        apart = jnp.arange(size) ^ place
        slots, others_slots = places(apart, falling), places(apart, crossed)
    else:
        width = 512 if cols % 512 == 0 else cols
        slots = others_slots = jnp.arange(cols // width)
        q_stack = lax.all_gather(q_own, "fsdp", axis=0, tiled=True).reshape(-1, width, rank)
    scalars = jnp.concatenate([island[None], slots, others_slots]).astype(jnp.int32)
    slots = slots.astype(jnp.int32)
    blocks = slots.shape[0]

    raw, projected, gram = project(slots, grads, buffer, q_stack)
    if split:
        for bit in bits:
            gram = gram + swap(gram, bit)
        for bit in bits:
            half = projected.shape[0] // 2
            projected = projected[:half] + swap(projected[half:], bit)
    else:
        projected, gram = lax.psum((projected, gram), "fsdp")
    lower = jnp.linalg.cholesky(gram)
    upper_inverse = lax.linalg.triangular_solve(
        lower, jnp.eye(rank, dtype=f32), left_side=True, lower=True, transpose_a=True
    )
    factor = jnp.einsum(
        "kr,bkw->brw", upper_inverse, projected, precision=precise, preferred_element_type=f32
    ).astype(bf16)
    pieces = [from_island(factor, d) for d in range(1, n)]
    pieces = [factor, *pieces]

    basis = exact(raw, upper_inverse).astype(bf16)
    by_part = basis.reshape(n, parts, height, rank)
    others = []
    for d in range(1, n):
        wanted = lax.dynamic_index_in_dim(by_part[:, -1], (island + n - d) % n, 0)
        sent = jnp.concatenate([by_part[:, 0], wanted], 0) if parts == 2 else wanted
        others.append(from_island(sent, d))

    if parts == 2 and forward:
        above, below = got
        down, up = onward(above, below)
        got = [(above,), (down, up), (below,)]
    elif parts == 2:
        got = [(piece,) for piece in got]
    stacks = [jnp.concatenate(pieces[:2], axis=1), jnp.concatenate(pieces[2:], axis=1)]
    if split:
        for pair in zip(falling, crossed):
            stacks = [spread(x, [bit]) for x, bit in zip(stacks, pair)]
    squares = [jnp.sum(jnp.square(x.astype(f32)), axis=(0, 2)) for x in stacks]
    scale = ((rate / n) / jnp.sqrt(jnp.concatenate(squares) + epsilon))[None]

    first, filled = [], []
    count = 2 if forward and blocks % 2 == 0 else 1
    for k in range(count):
        span = (k * blocks // count, (k + 1) * blocks // count)
        *filled, share = late(
            scalars, by_part, others, scale, stacks, momentum, anchor, span, filled
        )
        if forward:
            first.append(line_step(share, share, 1))
    low, *_ = tie(stacks[0], share)
    buffer_new = residue(slots, grads, buffer, basis, low)
    found = {}
    if forward:
        (*flat, buffer_new) = tie(*first[0], buffer_new)
        second = [line_step(*flat, 2)]
    if parts == 2:
        filled = early(
            scalars, by_part, others, scale, stacks, momentum, anchor, got, filled
        )
    momentum_new, anchor_new = filled
    if forward:
        if count == 2:
            (*flat, anchor_new) = tie(*first[1], anchor_new)
            second.append(line_step(*flat, 2))
        third = []
        for pair in second:
            third.append(line_step(*pair, 3))
        for d, (down, up) in ((1, (first, third)), (2, (second, second)), (3, (third, first))):
            found[d] = [x[0] + y[1] for x, y in zip(down, up)]
    else:
        found = {d: [from_island(share, d)] for d in range(1, n)}
    for k in range(count):
        for d in found:
            anchor_new = lax.dynamic_update_slice(
                anchor_new,
                found[d][k][None, None],
                ((island + d) % n, parts - 1, 0, k * cols // count),
            )
    return (
        anchor_new.reshape(rows, cols),
        buffer_new[None],
        momentum_new.reshape(quarter, cols),
    )


def solution(mesh):
    in_specs = (
        P("island", None, "fsdp", None),
        P("island", "fsdp", None),
        P("island", "fsdp", None),
        P("fsdp", None),
        P(("fsdp", "island"), None),
    )
    out_specs = (P("fsdp", None), P("island", "fsdp", None), P(("fsdp", "island"), None))

    return jax.shard_map(body, mesh=mesh, in_specs=in_specs, out_specs=out_specs, check_vma=False)
```

```python
import functools
import math

import jax
import jax.numpy as jnp
from jax import lax
from jax.experimental import pallas as pl
from jax.experimental.pallas import tpu as pltpu
from jax.sharding import PartitionSpec as P


precise = lax.Precision.HIGHEST
error_decay = 0.95
outer_beta = 0.9
outer_rate = 0.7
epsilon = 1e-06
EARLY = (3, 7)
CUTS = 1
bf16 = jnp.bfloat16
f32 = jnp.float32


def params(mib):
    return pltpu.CompilerParams(
        dimension_semantics=("arbitrary",), vmem_limit_bytes=mib * 1024 * 1024
    )


def cost(flops, moved):
    return pl.CostEstimate(flops=int(flops), bytes_accessed=int(moved), transcendentals=0)


def piece(shape, index):
    return pl.BlockSpec(tuple(pl.Element(size) for size in shape), index)


def divisor(total, most, step):
    return max(d for d in range(step, most + 1, step) if total % d == 0)


def project_kernel(slots, g_ref, b_ref, q_ref, raw_ref, proj_ref, gram_ref, q_scratch):
    blocks, width, _ = q_ref.shape

    @pl.when(pl.program_id(0) == 0)
    def _():
        proj_ref[...] = jnp.zeros_like(proj_ref)
        gram_ref[...] = jnp.zeros_like(gram_ref)
        for j in range(blocks):
            q_scratch[j * width : (j + 1) * width, :] = q_ref[slots[j]]

    matrix = g_ref[...] + b_ref[...]
    raw = jnp.dot(matrix, q_scratch[...], preferred_element_type=f32)
    raw_ref[...] = raw
    turned = raw.T
    gram_ref[...] += jnp.dot(turned, raw, precision=precise, preferred_element_type=f32)
    turned = turned.astype(bf16)
    for j in range(blocks):
        proj_ref[slots[j]] += jnp.dot(
            turned, matrix[:, j * width : (j + 1) * width], preferred_element_type=f32
        )


def project(slots, grads, buffer, q_stack):
    rows, cols = grads.shape
    blocks, width, rank = q_stack.shape
    step = divisor(rows, 256, 8)
    tile = pl.BlockSpec((step, cols), lambda i, s: (i, 0))
    whole = lambda shape: pl.BlockSpec(shape, lambda i, s: (0,) * len(shape))
    return pl.pallas_call(
        project_kernel,
        grid_spec=pltpu.PrefetchScalarGridSpec(
            num_scalar_prefetch=1,
            grid=(rows // step,),
            in_specs=[tile, tile, whole((blocks, width, rank))],
            out_specs=[
                pl.BlockSpec((step, rank), lambda i, s: (i, 0)),
                whole((blocks, rank, width)),
                whole((rank, rank)),
            ],
            scratch_shapes=[pltpu.VMEM((cols, rank), bf16)],
        ),
        out_shape=[
            jax.ShapeDtypeStruct((rows, rank), f32),
            jax.ShapeDtypeStruct((blocks, rank, width), f32),
            jax.ShapeDtypeStruct((rank, rank), f32),
        ],
        compiler_params=params(48),
        cost_estimate=cost(4 * rows * cols * rank, 4 * rows * cols),
        name="project",
    )(slots, grads, buffer, q_stack)


def residue_kernel(slots, g_ref, b_ref, p_ref, r_ref, out_ref):
    blocks, _, width = r_ref.shape
    basis = p_ref[...]
    for j in range(blocks):
        at = slice(j * width, (j + 1) * width)
        update = jnp.dot(basis, r_ref[slots[j]], preferred_element_type=f32)
        matrix = g_ref[:, at].astype(f32) + b_ref[:, at].astype(f32)
        out_ref[:, at] = (matrix - (1.0 - error_decay) * update).astype(bf16)


def residue(slots, grads, buffer, basis, stack):
    rows, cols = grads.shape
    blocks, _, width = stack.shape
    rank = basis.shape[1]
    step = divisor(rows, 256, 8)
    tile = pl.BlockSpec((step, cols), lambda i, s: (i, 0))
    return pl.pallas_call(
        residue_kernel,
        grid_spec=pltpu.PrefetchScalarGridSpec(
            num_scalar_prefetch=1,
            grid=(rows // step,),
            in_specs=[
                tile,
                tile,
                pl.BlockSpec((step, rank), lambda i, s: (i, 0)),
                pl.BlockSpec((blocks, rank, width), lambda i, s: (0, 0, 0)),
            ],
            out_specs=tile,
        ),
        out_shape=jax.ShapeDtypeStruct((rows, cols), bf16),
        compiler_params=params(48),
        cost_estimate=cost(2 * rows * cols * rank, 6 * rows * cols),
        name="residue",
    )(slots, grads, buffer, basis, stack)


def outer(momentum, anchor, mean):
    momentum_new = outer_beta * momentum + mean
    anchor_new = anchor.astype(f32) - outer_rate * (mean + outer_beta * momentum_new)
    return momentum_new, anchor_new.astype(bf16)


def scaled(rows, scale):
    return (rows.astype(f32) * scale).astype(bf16)


def change(left, low_ref, high_ref):
    depth = low_ref.shape[1]
    return jnp.dot(left[:, :depth], low_ref[0], preferred_element_type=f32) + jnp.dot(
        left[:, depth:], high_ref[0], preferred_element_type=f32
    )


def late_kernel(n, scalars, *refs):
    p_refs, (scale, low, high, m_ref, a_ref), refs = refs[:n], refs[n : n + 5], refs[n + 5 :]
    m_out, a_out, share, left = refs[-4:]
    rank = p_refs[0].shape[-1]

    @pl.when(pl.program_id(0) == 0)
    def _():
        for d in range(n):
            at = slice(d * rank, (d + 1) * rank)
            left[:, at] = scaled(p_refs[d][0] if d == 0 else p_refs[d][...], scale[:, at])

    momentum_new, anchor_new = outer(m_ref[...], a_ref[0], change(left, low, high))
    m_out[...] = momentum_new
    a_out[0] = anchor_new
    share[...] = anchor_new


def stack_specs(stacks, start):
    blocks = stacks[0].shape[0]
    return [
        pl.BlockSpec(
            (1, *stack.shape[1:]), lambda j, s, k=k: (s[1 + k * blocks + start + j], 0, 0)
        )
        for k, stack in enumerate(stacks)
    ]


def late(scalars, own, others, scale, stacks, momentum, anchor, offset, span, filled):
    n, quarter, _ = anchor.shape
    height = quarter - offset
    width, depth, rank = stacks[0].shape[-1], scale.shape[-1], own.shape[-1]
    start, stop = span
    fixed = lambda *at: (lambda j, s: at)
    column = lambda j: (start + j) * width
    m_spec = piece((height, width), lambda j, s: (offset, column(j)))
    a_spec = piece((1, height, width), lambda j, s: (s[0], offset, column(j)))
    columns = (stop - start) * width
    return pl.pallas_call(
        functools.partial(late_kernel, n),
        grid_spec=pltpu.PrefetchScalarGridSpec(
            num_scalar_prefetch=1,
            grid=(stop - start,),
            in_specs=[piece((1, height, rank), lambda j, s: (s[0], offset, 0))]
            + [piece((height, rank), fixed(n * offset, 0))] * (n - 1)
            + [pl.BlockSpec((1, depth), fixed(0, 0)), *stack_specs(stacks, start), m_spec, a_spec]
            + [pl.BlockSpec(memory_space=pl.ANY)] * len(filled),
            out_specs=[m_spec, a_spec, pl.BlockSpec((height, width), lambda j, s: (0, j))],
            scratch_shapes=[pltpu.VMEM((height, depth), bf16)],
        ),
        out_shape=[
            jax.ShapeDtypeStruct(momentum.shape, f32),
            jax.ShapeDtypeStruct(anchor.shape, bf16),
            jax.ShapeDtypeStruct((height, columns), bf16),
        ],
        input_output_aliases={n + 6 + k: k for k in range(len(filled))},
        compiler_params=params(48),
        cost_estimate=cost(2 * height * columns * depth, 14 * height * columns),
        name="late",
    )(scalars, own, *others, scale, *stacks, momentum, anchor, *filled)


def early_kernel(n, counts, scalars, *refs):
    p_refs, refs = refs[:n], refs[n:]
    (scale, low, high, m_ref, a_ref), refs = refs[:5], refs[5:]
    got, refs = refs[: sum(counts)], refs[sum(counts) :]
    _, _, m_out, a_out, left, mean = refs
    rank, height = p_refs[0].shape[-1], p_refs[0].shape[-2]

    @pl.when(pl.program_id(0) == 0)
    def _():
        for d in range(n):
            at = slice(d * rank, (d + 1) * rank)
            for k in range(n):
                to = slice(k * height, (k + 1) * height)
                left[to, at] = scaled(p_refs[d][k] if d == 0 else p_refs[d][to], scale[:, at])

    mean[...] = change(left, low, high).reshape(mean.shape)
    for d in range(n):
        k = lax.rem(scalars[0] + d, n)
        if d == 0:
            momentum = m_ref[...]
        else:
            start = sum(counts[: d - 1])
            momentum = got[start][...].astype(f32)
            for ref in got[start + 1 : start + counts[d - 1]]:
                momentum = momentum + ref[...].astype(f32)
        momentum_new, anchor_new = outer(momentum, a_ref[k], mean[k])
        if d == 0:
            m_out[...] = momentum_new
        a_out[k] = anchor_new


def early(scalars, own, others, scale, stacks, momentum, anchor, height, got, span, filled):
    n, _, _ = anchor.shape
    width, (start, stop) = stacks[0].shape[-1], span
    depth, rank = scale.shape[-1], own.shape[-1]
    counts = [len(pieces) for pieces in got]
    flat = [piece for pieces in got for piece in pieces]
    fixed = lambda *at: (lambda j, s: at)
    column = lambda j: (start + j) * width
    m_spec = piece((height, width), lambda j, s: (0, column(j)))
    a_spec = piece((n, height, width), lambda j, s: (0, 0, column(j)))
    first_alias = n + 6 + len(flat)
    return pl.pallas_call(
        functools.partial(early_kernel, n, counts),
        grid_spec=pltpu.PrefetchScalarGridSpec(
            num_scalar_prefetch=1,
            grid=(stop - start,),
            in_specs=[piece((n, height, rank), fixed(0, 0, 0))]
            + [piece((n * height, rank), fixed(0, 0))] * (n - 1)
            + [pl.BlockSpec((1, depth), fixed(0, 0)), *stack_specs(stacks, start), m_spec, a_spec]
            + [pl.BlockSpec((height, width), lambda j, s: (0, j))] * len(flat)
            + [pl.BlockSpec(memory_space=pl.ANY)] * 2,
            out_specs=[m_spec, a_spec],
            scratch_shapes=[
                pltpu.VMEM((n * height, depth), bf16),
                pltpu.VMEM((n, height, width), f32),
            ],
        ),
        out_shape=[
            jax.ShapeDtypeStruct(momentum.shape, f32),
            jax.ShapeDtypeStruct(anchor.shape, bf16),
        ],
        input_output_aliases={first_alias: 0, first_alias + 1: 1},
        compiler_params=params(56),
        cost_estimate=cost(
            2 * n * height * (stop - start) * width * depth, 32 * height * (stop - start) * width
        ),
        name="early",
    )(scalars, own, *others, scale, *stacks, momentum, anchor, *flat, *filled)


def swap(x, bit):
    size = lax.axis_size("fsdp")
    return lax.ppermute(x, "fsdp", [(i, i ^ bit) for i in range(size)])


def spread(x, bits):
    for bit in bits:
        x = jnp.concatenate([x, swap(x, bit)], axis=0)
    return x


def places(apart, bits):
    return functools.reduce(
        jnp.bitwise_or,
        [((apart >> bit.bit_length() - 1) & 1) << k for k, bit in enumerate(bits)],
        jnp.zeros_like(apart),
    )


def from_island(x, ahead):
    n = lax.axis_size("island")
    return lax.ppermute(x, "island", [(s, (s - ahead) % n) for s in range(n)])


def near(x):
    return from_island(x, 1), from_island(x, lax.axis_size("island") - 1)


def onward(above, below):
    down = lax.ppermute(above, "island", [(1, 0), (2, 1)])
    up = lax.ppermute(below, "island", [(1, 2), (2, 3)])
    return down, up


def line_step(down, up, step):
    n = lax.axis_size("island")
    down = lax.ppermute(down, "island", [(k, k - 1) for k in range(1, n - step + 1)])
    up = lax.ppermute(up, "island", [(k, k + 1) for k in range(step - 1, n - 1)])
    return down, up


def tie(*values):
    return lax.optimization_barrier(values)


def exact(a, b):
    return jnp.dot(a, b, precision=precise, preferred_element_type=f32)


def body(grads, buffer, q_old, anchor, momentum):
    n, size = lax.axis_size("island"), lax.axis_size("fsdp")
    island, place = lax.axis_index("island"), lax.axis_index("fsdp")
    grads, buffer, q_old = grads[0, 0], buffer[0], q_old[0]
    rows, cols = grads.shape
    rank = q_old.shape[1]
    rate = math.sqrt(rows * size * cols / rank)

    quarter = momentum.shape[0]
    forward = n == 4
    offset = quarter * EARLY[0] // EARLY[1] // 16 * 16 if forward else 0
    anchor = anchor.reshape(n, quarter, cols)
    count = 2 if forward and cols % 2048 == 0 else 1
    got = []
    cuts = CUTS if count == CUTS else 1
    for k in range(cuts if offset else 0):
        at = slice(k * cols // cuts, (k + 1) * cols // cuts)
        got.append(near(momentum[:offset, at].astype(bf16)))

    bits = [1 << k for k in range(size.bit_length() - 1)]
    split = size == 1 << len(bits) and (cols // size) % 128 == 0
    q_own = q_old.astype(bf16)
    if split:
        falling = bits[::-1]
        crossed = falling[1::-1] + falling[2:]
        q_stack = spread(q_own[None], falling)
        apart = jnp.arange(size) ^ place
        slots, others_slots = places(apart, falling), places(apart, crossed)
    else:
        width = 512 if cols % 512 == 0 else cols
        slots = others_slots = jnp.arange(cols // width)
        q_stack = lax.all_gather(q_own, "fsdp", axis=0, tiled=True).reshape(-1, width, rank)
    scalars = jnp.concatenate([island[None], slots, others_slots]).astype(jnp.int32)
    slots = slots.astype(jnp.int32)
    blocks = slots.shape[0]

    raw, projected, gram = project(slots, grads, buffer, q_stack)
    if split:
        for bit in bits:
            gram = gram + swap(gram, bit)
        for bit in bits:
            half = projected.shape[0] // 2
            projected = projected[:half] + swap(projected[half:], bit)
    else:
        projected, gram = lax.psum((projected, gram), "fsdp")
    lower = jnp.linalg.cholesky(gram)
    upper_inverse = lax.linalg.triangular_solve(
        lower, jnp.eye(rank, dtype=f32), left_side=True, lower=True, transpose_a=True
    )
    factor = jnp.einsum(
        "kr,bkw->brw", upper_inverse, projected, precision=precise, preferred_element_type=f32
    ).astype(bf16)
    pieces = [from_island(factor, d) for d in range(1, n)]
    pieces = [factor, *pieces]

    basis = exact(raw, upper_inverse).astype(bf16)
    rows_of = basis.reshape(n, quarter, rank)
    others = []
    for d in range(1, n):
        to = (island + n - d) % n
        wanted = lax.dynamic_slice(rows_of, (to, offset, 0), (1, quarter - offset, rank))[0]
        ahead = rows_of[:, :offset].reshape(n * offset, rank)
        others.append(from_island(jnp.concatenate([ahead, wanted], 0), d))

    for k, (above, below) in enumerate(got):
        down, up = onward(above, below)
        got[k] = [(above,), (down, up), (below,)]
    stacks = [jnp.concatenate(pieces[:2], axis=1), jnp.concatenate(pieces[2:], axis=1)]
    if split:
        for pair in zip(falling, crossed):
            stacks = [spread(x, [bit]) for x, bit in zip(stacks, pair)]
    squares = [jnp.sum(jnp.square(x.astype(f32)), axis=(0, 2)) for x in stacks]
    scale = ((rate / n) / jnp.sqrt(jnp.concatenate(squares) + epsilon))[None]

    first, filled = [], []
    spans = [(k * blocks // count, (k + 1) * blocks // count) for k in range(count)]
    for span in spans:
        *filled, share = late(
            scalars, rows_of, others, scale, stacks, momentum, anchor, offset, span, filled
        )
        if forward:
            first.append(line_step(share, share, 1))
    low, *_ = tie(stacks[0], share)
    buffer_new = residue(slots, grads, buffer, basis, low)
    found = {}
    if forward:
        (*flat, buffer_new) = tie(*first[0], buffer_new)
        second = [line_step(*flat, 2)]
    spans = [(k * blocks // cuts, (k + 1) * blocks // cuts) for k in range(cuts)]
    for pieces, span in zip(got, spans):
        filled = early(
            scalars, rows_of, others, scale, stacks, momentum, anchor, offset, pieces, span, filled
        )
    momentum_new, anchor_new = filled
    if forward:
        if count == 2:
            (*flat, anchor_new) = tie(*first[1], anchor_new)
            second.append(line_step(*flat, 2))
        third = []
        for pair in second:
            third.append(line_step(*pair, 3))
        for d, (down, up) in ((1, (first, third)), (2, (second, second)), (3, (third, first))):
            found[d] = [x[0] + y[1] for x, y in zip(down, up)]
    else:
        found = {d: [from_island(share, d)] for d in range(1, n)}
    for k in range(count):
        for d in found:
            anchor_new = lax.dynamic_update_slice(
                anchor_new,
                found[d][k][None],
                ((island + d) % n, offset, k * cols // count),
            )
    return (
        anchor_new.reshape(rows, cols),
        buffer_new[None],
        momentum_new,
    )


def solution(mesh):
    in_specs = (
        P("island", None, "fsdp", None),
        P("island", "fsdp", None),
        P("island", "fsdp", None),
        P("fsdp", None),
        P(("fsdp", "island"), None),
    )
    out_specs = (P("fsdp", None), P("island", "fsdp", None), P(("fsdp", "island"), None))

    return jax.shard_map(body, mesh=mesh, in_specs=in_specs, out_specs=out_specs, check_vma=False)
```
